32 devices in a mesh: rows: 8 (over y, x, core), cols: 4 (over z).
Axes of the slice: x: 2, y: 2, z: 4, core: 2. Of those that a mesh axis runs over, the one named last changes fastest.
Arguments:
- density: bfloat16 [640, 640], P('rows', 'cols'), as said below
- occupancy: int32 [5, 5], replicated, may hold values from 0 to 1, as said below
- square_filter: int32 [5, 5], replicated, may hold values 0 or 1
- cube_filter: int32 [5, 5], replicated, may hold values 0 or 1
Outputs:
- purified: float32 [640, 640], P('rows', 'cols')
The draws below stay inside these ranges and needn't reach their ends.
Inputs may be any that keep to these rules, and one draw needn't show every extreme that they name: density is symmetric. occupancy is symmetric and every diagonal tile is stored.
All inputs are finite; a program needn't handle non-finite values.
Results may differ from the reference program's by a relative error of at most 0.0095.
Values may be sent and summed in bfloat16 or wider, within the bound.
A program may use at most 64 MiB of HBM per device.

```python
import jax
import jax.numpy as jnp
from jax import lax

TILE = 128
N = 640
NT = 5


def draw_density(key, part):
    first = jax.random.fold_in(key, 0)
    base = jax.random.normal(first, (N, N), jnp.float32)
    symmetric = (base + base.T) * 0.5 ** 0.5 / (0.4 * N) ** 0.5
    return symmetric.astype(jnp.bfloat16)


def draw_occupancy(key, part):
    draws = jax.random.randint(key, (NT, NT), 0, 1000)
    summed = draws + draws.T
    indices = jnp.arange(NT)
    gap = jnp.abs(indices[:, None] - indices[None, :])
    distance = jnp.minimum(gap, NT - gap)
    halfway = max(NT // 2, 1)
    limit = 1600 - 1200 * distance // halfway
    stored = (summed < limit) | (gap == 0)
    return stored.astype(jnp.int32)


def place_ends(array, own_key, smallest, largest):
    spot = [jax.random.randint(jax.random.fold_in(own_key, axis), (), 0, length) for axis, length in enumerate(array.shape)]
    longest = array.shape.index(max(array.shape))
    next_to = spot[:longest] + [(spot[longest] + 1) % array.shape[longest]] + spot[longest + 1:]
    return array.at[tuple(spot)].set(smallest).at[tuple(next_to)].set(largest)


def setup_inputs(seed: int = 0) -> dict:
    keys = jax.random.split(jax.random.key(seed), 5)
    return {
        "density": draw_density(jax.random.fold_in(keys[4], 71), 0),
        "occupancy": draw_occupancy(jax.random.fold_in(keys[4], 71), 0),
        "square_filter": place_ends((jax.random.randint(keys[2], (NT, NT), 0, 4) < 3).astype(jnp.int32), jax.random.fold_in(keys[2], 1), 0, 1),
        "cube_filter": place_ends((jax.random.randint(keys[3], (NT, NT), 0, 4) < 3).astype(jnp.int32), jax.random.fold_in(keys[3], 1), 0, 1),
    }


def expand(table):
    return jnp.repeat(jnp.repeat(table, TILE, axis=0), TILE, axis=1)


def reference(density, occupancy, square_filter, cube_filter):
    occupied = jnp.where(expand(occupancy) > 0, density, jnp.zeros_like(density))
    values = occupied.astype(jnp.float32)
    square_total = jnp.dot(values, values, precision=lax.Precision.HIGHEST)
    square = jnp.where(expand(square_filter) > 0, square_total, jnp.zeros_like(square_total)).astype(jnp.bfloat16)
    cube_total = jnp.dot(square.astype(jnp.float32), values, precision=lax.Precision.HIGHEST)
    cube = jnp.where(expand(cube_filter) > 0, cube_total, jnp.zeros_like(cube_total))
    return 3.0 * square.astype(jnp.float32) - 2.0 * cube
```

```python
import functools

import jax
import jax.numpy as jnp
from jax import lax
from jax.experimental import pallas as pl
from jax.experimental.pallas import tpu as pltpu
from jax.sharding import PartitionSpec as P

TILE = 128
MESH = pl.DeviceIdType.MESH


def tiles_touched(blocks, size):
    return max(((b + 1) * size - 1) // TILE - b * size // TILE + 1 for b in range(blocks))


def mask_of(table, r, c, nr, nc, h, w):
    last = table.shape[0] - 1
    row_start, col_start = r * h, c * w
    row_tile, col_tile = row_start // TILE, col_start // TILE
    rows = row_start - row_tile * TILE + lax.broadcasted_iota(jnp.int32, (h, w), 0)
    cols = col_start - col_tile * TILE + lax.broadcasted_iota(jnp.int32, (h, w), 1)
    row_tiles, col_tiles = tiles_touched(nr, h), tiles_touched(nc, w)

    def row_values(i):
        tile = jnp.minimum(row_tile + i, last)
        value = jnp.full((h, w), table[tile, jnp.minimum(col_tile + col_tiles - 1, last)], jnp.int32)
        for j in range(col_tiles - 2, -1, -1):
            value = jnp.where(cols < (j + 1) * TILE, table[tile, col_tile + j], value)
        return value

    value = row_values(row_tiles - 1)
    for i in range(row_tiles - 2, -1, -1):
        value = jnp.where(rows < (i + 1) * TILE, row_values(i), value)
    return value > 0


def kernel(
    nr, nc, density, occupancy, square_filter, cube_filter, out,
    own, square, panel, column, squares,
    row_send, row_recv, col_send, col_recv, sq_send, sq_recv,
):
    r, c = lax.axis_index("rows"), lax.axis_index("cols")
    h, w = density.shape
    per = nr // nc

    barrier = pltpu.get_barrier_semaphore()
    row_peers = [lax.rem(c + d, nc) for d in range(1, nc)]
    col_peers = [lax.rem(r + d, nr) for d in range(1, nr)]
    for p in row_peers:
        pl.semaphore_signal(barrier, inc=1, device_id=(r, p), device_id_type=MESH)
    for p in col_peers:
        pl.semaphore_signal(barrier, inc=1, device_id=(p, c), device_id_type=MESH)

    stored = mask_of(occupancy, r, c, nr, nc, h, w)
    mine = jnp.where(stored, density[...].astype(jnp.float32), 0.0).astype(jnp.bfloat16)
    own[...] = mine
    panel[c] = mine
    column[r] = mine
    square_mask = mask_of(square_filter, r, c, nr, nc, h, w)

    pl.semaphore_wait(barrier, nr + nc - 2)

    sends = []
    for d, p in enumerate(row_peers):
        sends.append(pltpu.make_async_remote_copy(
            own, panel.at[c], row_send.at[d], row_recv.at[d], device_id=(r, p), device_id_type=MESH))
    for d, p in enumerate(col_peers):
        sends.append(pltpu.make_async_remote_copy(
            own, column.at[r], col_send.at[d], col_recv.at[d], device_id=(p, c), device_id_type=MESH))
    for s in sends:
        s.start()
    for d in range(nc - 1):
        src = lax.rem(c + nc - 1 - d, nc)
        pltpu.make_async_remote_copy(
            own, panel.at[src], row_send.at[d], row_recv.at[d], device_id=(r, src), device_id_type=MESH).wait_recv()
    for d in range(nr - 1):
        src = lax.rem(r + nr - 1 - d, nr)
        pltpu.make_async_remote_copy(
            own, column.at[src], col_send.at[d], col_recv.at[d], device_id=(src, c), device_id_type=MESH).wait_recv()

    def columns_at(k):
        return column[pl.ds(k * per, per)].reshape(per * h, w)

    total = jnp.zeros((h, w), jnp.float32)
    for k in range(nc):
        total += jnp.dot(panel[k], columns_at(k), preferred_element_type=jnp.float32)
    mine2 = jnp.where(square_mask, total, 0.0).astype(jnp.bfloat16)
    square[...] = mine2
    sq = []
    for d, p in enumerate(row_peers):
        sq.append(pltpu.make_async_remote_copy(
            square, squares.at[d], sq_send.at[d], sq_recv.at[d], device_id=(r, p), device_id_type=MESH))
    for s in sq:
        s.start()
    cube = jnp.dot(mine2, columns_at(c), preferred_element_type=jnp.float32)
    cube_mask = mask_of(cube_filter, r, c, nr, nc, h, w)
    for d in range(nc - 1):
        src = lax.rem(c + nc - 1 - d, nc)
        sq[d].wait_recv()
        cube += jnp.dot(squares[d], columns_at(src), preferred_element_type=jnp.float32)
    out[...] = 3.0 * mine2.astype(jnp.float32) - 2.0 * jnp.where(cube_mask, cube, 0.0)
    for s in sends + sq:
        s.wait_send()


def solution(mesh):
    nr, nc = mesh.shape["rows"], mesh.shape["cols"]

    def step(density, occupancy, square_filter, cube_filter):
        h, w = density.shape
        bf = jnp.bfloat16
        return pl.pallas_call(
            functools.partial(kernel, nr, nc),
            out_shape=jax.ShapeDtypeStruct((h, w), jnp.float32),
            in_specs=[pl.BlockSpec(memory_space=pltpu.VMEM)]
            + [pl.BlockSpec(memory_space=pltpu.SMEM)] * 3,
            out_specs=pl.BlockSpec(memory_space=pltpu.VMEM),
            scratch_shapes=[
                pltpu.VMEM((h, w), bf),
                pltpu.VMEM((h, w), bf),
                pltpu.VMEM((nc, h, w), bf),
                pltpu.VMEM((nr, h, w), bf),
                pltpu.VMEM((nc - 1, h, w), bf),
                pltpu.SemaphoreType.DMA((nc - 1,)),
                pltpu.SemaphoreType.DMA((nc - 1,)),
                pltpu.SemaphoreType.DMA((nr - 1,)),
                pltpu.SemaphoreType.DMA((nr - 1,)),
                pltpu.SemaphoreType.DMA((nc - 1,)),
                pltpu.SemaphoreType.DMA((nc - 1,)),
            ],
            compiler_params=pltpu.CompilerParams(collective_id=0, has_side_effects=True),
        )(density, occupancy, square_filter, cube_filter)

    placed = (P("rows", "cols"), P(), P(), P())
    return jax.shard_map(
        step, mesh=mesh, in_specs=placed, out_specs=P("rows", "cols"), check_vma=False
    )
```
